128 devices in a mesh: seq: 8 (over z, core), exp: 16 (over y, x).
Axes of the slice: x: 4, y: 4, z: 4, core: 2. Of those that a mesh axis runs over, the one named last changes fastest.
Arguments:
- tokens: bfloat16 [81920, 4096], P(('seq', 'exp')), may hold values from -6 to 6
- routes: int32 [81920, 2], P(('seq', 'exp')), may hold values from 0 to 31, all different within a row; in each aligned block of 640 rows (0 to 639, 640 to 1279, ...) at most 50 rows name the same one
- gates: float32 [81920, 2], P(('seq', 'exp')), may hold values from 0.1 to 1
- weights: bfloat16 [32, 4096, 1024], P('exp', 'seq'), may hold values from -0.09375 to 0.09375
Outputs:
- mixed: bfloat16 [81920, 1024], P(('seq', 'exp'))
The draws below stay inside these ranges and needn't reach their ends.
Inputs may be any that keep to these rules, and one draw needn't show every extreme that they name: `routes`: the two experts of a token differ. Among the rows of one device no expert is named more than 50 times, a bound that some block reaches.
All inputs are finite; a program needn't handle non-finite values.
Results may differ from the reference program's by a relative error of at most 0.0049.
Values may be sent and summed in bfloat16 or wider, within the bound.
No kernel may reach another device: no remote copies, remote signals or barrier semaphores. Data moves between devices by JAX's collectives and lax.ppermute only.
A program may use at most 192 MiB of HBM per device.

```python
import math
import jax
import jax.numpy as jnp
import numpy as np
from jax import lax

D = 4096
FF = 1024
TOK_DEV = 640
EXPERTS = 32
CAP = 50
TOKENS = 81920


def levels(rng, shape, shards, low, high):
    factor_of = 1.0
    for dim, shards_of in shards:
        draws = jax.random.uniform(jax.random.fold_in(jax.random.fold_in(rng, 6), dim), (shards_of,), jnp.float32, low / len(shards), high / len(shards))
        factor_of = factor_of * jnp.repeat(jnp.exp(draws), shape[dim] // shards_of).reshape((-1,) + (1,) * (len(shape) - 1 - dim))
    return factor_of


def deal_out(stream_key, own, number, rows, amount, top, limit, slope):
    sequence = jax.random.permutation(stream_key, amount)
    crowded, common = shares(amount, rows * top, limit, slope, True), shares(amount, rows * top, limit, slope, False)
    places = jnp.arange(amount)

    def named(lengths, turn):
        used = int((lengths > 0).sum())
        fixed = max(1, used // 4)
        shifted = fixed + (places - fixed + turn * (used - fixed)) % max(1, amount - fixed)
        return jnp.zeros((amount,), jnp.int32).at[sequence[jnp.where(places < fixed, places, shifted)]].set(jnp.asarray(lengths, jnp.int32))

    lengths = jnp.where(number % 4 == 0, named(crowded, number // 4), named(common, number - number // 4 - 1))
    mixed = jax.random.permutation(jax.random.fold_in(own, 3), amount)
    donor, sink = mixed[0:amount // 2 * 2:2], mixed[1:amount // 2 * 2:2]
    margin = jnp.minimum(lengths[donor] - 1, limit - lengths[sink]) // 2
    margin = jnp.where((donor == sequence[0]) | (sink == sequence[0]) | (lengths[sink] == 0), 0, jnp.maximum(margin, 0))
    shifted = jax.random.randint(jax.random.fold_in(own, 4), (amount // 2,), 0, 1 << 20) % (margin + 1)
    lengths = lengths.at[donor].add(-shifted).at[sink].add(shifted)
    items = jnp.searchsorted(jnp.cumsum(lengths), jnp.arange(rows * top), side="right").astype(jnp.int32)
    grid = items.reshape(top, rows).T
    grid = grid[jax.random.permutation(jax.random.fold_in(own, 1), rows)]
    turn = jax.random.randint(jax.random.fold_in(own, 2), (rows, 1), 0, top)
    return jnp.take_along_axis(grid, (jnp.arange(top)[None, :] + turn) % top, axis=1)


def shares(number_of, total, most, skew, full):
    weights = [(1 << 20) // math.isqrt(standing ** skew) + 1 for standing in range(1, number_of + 1)]
    largest = most if full else min(most, max(-(-total // number_of), total * weights[0] // sum(weights)))
    least = 1 if total - largest >= number_of - 1 else 0
    holding, rest = [largest] + [least] * (number_of - 1), total - largest - least * (number_of - 1)
    while rest > 0:
        free = [i for i in range(1, number_of) if holding[i] < largest] or [i for i in range(1, number_of) if holding[i] < most]
        mass, budget = sum([weights[i] for i in free]), rest
        for i in free:
            more = min(most - holding[i], max(1, budget * weights[i] // mass), rest)
            holding[i] = holding[i] + more
            rest = rest - more
    return np.array(holding)


def scatter_about(rng, extent, scale, most, pieces=(), held_as=jnp.bfloat16):
    gain = levels(rng, extent, pieces, -0.22, 0.18) if pieces else 1.0
    drawn = jax.random.normal(rng, extent, jnp.float32) * scale * gain
    return jnp.minimum(jnp.maximum(drawn, -most), most).astype(held_as)


def setup_inputs(seed: int = 0) -> dict:
    seeds = jax.random.split(jax.random.key(seed), 5)
    tokens = scatter_about(seeds[0], (TOKENS, D), 1.0, 6.0, ((0, 128),))
    routes_keys = jax.random.split(jax.random.fold_in(seeds[1], 1), TOKENS // TOK_DEV)
    routes_turns = jax.random.permutation(jax.random.fold_in(seeds[1], 3), TOKENS // TOK_DEV)
    routes = jax.vmap(lambda own, number: deal_out(jax.random.fold_in(seeds[1], 2), own, number, TOK_DEV, EXPERTS, 2, CAP, 2))(routes_keys, routes_turns).reshape((TOKENS, 2))
    gates = jnp.clip(0.1 + 0.9 * jax.random.uniform(seeds[2], (TOKENS, 2), jnp.float32) ** levels(seeds[2], (TOKENS, 2), ((0, 128),), -0.2, 0.2), 0.1, 1.0)
    weights = scatter_about(seeds[3], (EXPERTS, D, FF), D ** -0.5, 0.09375, ((0, 16), (1, 8)))
    return dict(tokens=tokens, routes=routes, gates=gates, weights=weights)


def route_slots(route_block, experts, capacity):
    expert_ids = route_block.reshape(-1)
    one_hot = (expert_ids[:, None] == jnp.arange(experts, dtype=jnp.int32)[None, :]).astype(jnp.int32)
    earlier = jnp.cumsum(one_hot, axis=0) - one_hot
    slot_index = jnp.sum(earlier * one_hot, axis=1)
    return (expert_ids * capacity + slot_index).astype(jnp.int32)


def reference(tokens, routes, gates, weights):
    blocks = TOKENS // TOK_DEV
    route_blocks = routes.reshape(blocks, TOK_DEV, 2)
    position = jax.vmap(lambda block: route_slots(block, EXPERTS, CAP))(route_blocks)
    local_rows = jnp.arange(2 * TOK_DEV, dtype=jnp.int32) // 2
    block_base = (jnp.arange(blocks, dtype=jnp.int32) * TOK_DEV)[:, None]
    global_rows = block_base + local_rows[None, :]

    def fill_table(places, rows):
        return jnp.full((EXPERTS * CAP,), TOKENS, jnp.int32).at[places].set(rows)

    slot_rows = jax.vmap(fill_table)(position, global_rows).reshape(blocks, EXPERTS, CAP)
    padded = jnp.concatenate([tokens, jnp.zeros((1, D), jnp.bfloat16)], axis=0)

    def one_expert(expert):
        indices = lax.dynamic_index_in_dim(slot_rows, expert, 1, keepdims=False).reshape(-1)
        gathered = padded[indices]
        matrix = lax.dynamic_index_in_dim(weights, expert, 0, keepdims=False)
        return jnp.dot(gathered, matrix, preferred_element_type=jnp.float32).astype(jnp.bfloat16)

    outputs = lax.map(one_expert, jnp.arange(EXPERTS, dtype=jnp.int32))
    outputs = outputs.reshape(EXPERTS * blocks * CAP, FF)
    expert_ids = route_blocks.reshape(blocks, 2 * TOK_DEV)
    slot_index = position - expert_ids * CAP
    block_ids = jnp.arange(blocks, dtype=jnp.int32)[:, None]
    flat_index = ((expert_ids * blocks + block_ids) * CAP + slot_index).reshape(-1)
    picked = outputs[flat_index].reshape(TOKENS, 2, FF).astype(jnp.float32)
    mixed = jnp.sum(picked * gates[:, :, None], axis=1)
    return mixed.astype(jnp.bfloat16)
```

```python
import jax
import jax.numpy as jnp
from jax import lax
from jax.sharding import Mesh, PartitionSpec as P

CHUNKS = ((0, 2), (2, 32), (34, 16))
RETURNS = ((0, 1), (2,))


def gather_weights(weights):
    core = lax.axis_index("core")
    depth = weights.shape[1]
    z_size = lax.axis_size("z")
    mine = lax.dynamic_index_in_dim(weights, core, 0, keepdims=False)
    other = lax.dynamic_index_in_dim(weights, 1 - core, 0, keepdims=False)
    got = lax.ppermute(other, "core", [(0, 1), (1, 0)])
    own = jnp.where(core == 0, jnp.concatenate([mine, got]), jnp.concatenate([got, mine]))
    place = lax.axis_index("z")
    up = [(i, (i + 1) % z_size) for i in range(z_size)]
    down = [(j, i) for i, j in up]
    half = depth
    below = lax.ppermute(own, "z", up)
    above = lax.ppermute(own, "z", down)
    far_first = lax.ppermute(below[:half], "z", up)
    far_last = lax.ppermute(above[half:], "z", down)
    blocks = ((own, 0), (below, -1), (above, 1), (jnp.concatenate([far_first, far_last]), 2))
    whole = jnp.zeros((z_size * 2 * depth, weights.shape[2]), weights.dtype)
    for block, shift in blocks:
        at = ((place + shift) % z_size) * (2 * depth)
        whole = lax.dynamic_update_slice(whole, block, (at, 0))
    return whole


def body(tokens, routes, gates, weights):
    rows, width = tokens.shape
    groups = lax.axis_size("exp")
    cores = lax.axis_size("core")
    experts = groups * cores
    capacity = 5 * rows // (2 * experts)
    dest = jnp.arange(experts, dtype=jnp.int32)
    ids = (cores * (dest % groups) + dest // groups)[:, None]
    first, second = routes[:, 0][None, :], routes[:, 1][None, :]
    in_first, in_second = ids == first, ids == second
    named = in_first | in_second
    earlier = (
        lax.broadcasted_iota(jnp.int32, (rows, rows), 0)
        < lax.broadcasted_iota(jnp.int32, (rows, rows), 1)
    )
    rank = jnp.dot(
        named.astype(jnp.bfloat16), earlier.astype(jnp.bfloat16), preferred_element_type=jnp.float32
    ).astype(jnp.int32)
    slot = jnp.where(named, rank, -1)
    gate = jnp.where(in_first, gates[:, 0][None, :], jnp.where(in_second, gates[:, 1][None, :], 0.0))
    gate_hi = gate.astype(jnp.bfloat16)
    gate_lo = (gate - gate_hi.astype(jnp.float32)).astype(jnp.bfloat16)
    slot = slot[:, None, :]

    def chosen(start, size):
        return slot == (start + jnp.arange(size, dtype=jnp.int32))[None, :, None]

    whole = gather_weights(weights)
    axes = ("core", "exp")
    outs = []
    for start, size in CHUNKS:
        pick = chosen(start, size).astype(jnp.bfloat16).reshape(experts * size, rows)
        packed = jnp.dot(pick, tokens, preferred_element_type=jnp.float32).astype(jnp.bfloat16)
        packed = packed.reshape(experts, size, width)
        got = lax.all_to_all(packed, axes, split_axis=0, concat_axis=0, tiled=True)
        out = jnp.dot(
            got.reshape(experts * size, width), whole, preferred_element_type=jnp.float32
        ).astype(jnp.bfloat16)
        outs.append(out.reshape(experts, size, -1))
    mixed = 0.0
    for part in RETURNS:
        start = CHUNKS[part[0]][0]
        size = sum(CHUNKS[i][1] for i in part)
        sent = outs[part[0]] if len(part) == 1 else jnp.concatenate([outs[i] for i in part], axis=1)
        back = lax.all_to_all(sent, axes, split_axis=0, concat_axis=0, tiled=True)
        back = back.reshape(experts * size, -1)
        here = chosen(start, size)
        for gate_part in (gate_hi, gate_lo):
            weight = jnp.where(here, gate_part[:, None, :], jnp.bfloat16(0)).reshape(experts * size, rows)
            mixed = mixed + lax.dot_general(
                weight, back, (((0,), (0,)), ((), ())), preferred_element_type=jnp.float32
            )
    return mixed.astype(jnp.bfloat16)


def solution(mesh):
    cores = 2
    seq, exp = mesh.devices.shape
    fine = Mesh(mesh.devices.reshape(seq // cores, cores, exp), ("z", "core", "exp"))
    every = ("z", "core", "exp")
    return jax.shard_map(
        body,
        mesh=fine,
        in_specs=(P(every, None), P(every, None), P(every, None), P("exp", ("z", "core"), None)),
        out_specs=P(every, None),
        check_vma=False,
    )
```

```python
import functools

import jax
import jax.numpy as jnp
import numpy as np
from jax import lax
from jax.experimental import pallas as pl
from jax.experimental.pallas import tpu as pltpu
from jax.sharding import Mesh, PartitionSpec as P

CORES = 2
SIDE = 4
LOOSE = 2
PLANE = ("core", "y", "x")
SETS = (((0, 0), (1, 1)), ((0, -1), (-1, 2)))
BLOCKS = SETS[0] + SETS[1]
EXPERT_CALLS = (((1, 3, 2, 0),), ((1, 3), (2, 0)))
INTERPRET = False


def flat(core, y, x):
    return (core * SIDE + y % SIDE) * SIDE + x % SIDE


def pairs(first, second):
    out = []
    for core in range(CORES):
        dy, dx = (second, first) if core == 0 else (first, second)
        for y in range(SIDE):
            for x in range(SIDE):
                out.append((flat(core, y, x), flat(core, y + dy, x + dx)))
    return out


def crossed(moves):
    side = SIDE * SIDE
    return [(source, (1 - target // side) * side + target % side) for source, target in moves]


def back(moves):
    return [(target, source) for source, target in moves]


SWAP = [(0, 1), (1, 0)]
SHIFTS = (0, SIDE - 1, 1, 2)
PARTS = 2 * SIDE
UP = [(i, (i + 1) % SIDE) for i in range(SIDE)]


def regroup_kernel(main, *refs):
    ins, outs = refs[:SIDE], refs[SIDE:]
    for i, source in enumerate(ins):
        for j, target in enumerate(outs):
            target[i * main : (i + 1) * main] = source[j * main : (j + 1) * main]
    rest = SIDE * main
    for j, target in enumerate(outs):
        tail = [source[rest + j * LOOSE : rest + (j + 1) * LOOSE] for source in ins]
        target[rest:] = jnp.concatenate(tail + [source_pad(target, rest)], axis=0)


def source_pad(target, rest):
    rows = target.shape[0] - rest - SIDE * LOOSE
    return jnp.zeros((rows, target.shape[1]), target.dtype)


def regroup(arrays, main):
    rows, width = arrays[0].shape
    step = min(width, 1024)
    spec = pl.BlockSpec((rows, step), lambda i: (0, i))
    size = SIDE * rows * width * 2
    return pl.pallas_call(
        functools.partial(regroup_kernel, main),
        grid=(width // step,),
        in_specs=[spec] * SIDE,
        out_specs=[spec] * SIDE,
        out_shape=[jax.ShapeDtypeStruct((rows, width), arrays[0].dtype)] * SIDE,
        cost_estimate=pl.CostEstimate(flops=size, bytes_accessed=2 * size, transcendentals=0),
        interpret=INTERPRET,
        name="regroup",
    )(*arrays)


def dispatch_kernel(spread_ref, row_slot_ref, slot_ref, tokens_ref, *refs):
    outs, pick_ref = refs[:-1], refs[-1]
    length = outs[0].shape[0]

    @pl.when(pl.program_id(0) == 0)
    def _():
        at_row = jnp.dot(spread_ref[...], slot_ref[...], preferred_element_type=jnp.float32)
        pick_ref[...] = jnp.where(at_row == row_slot_ref[...], 1.0, 0.0).astype(pick_ref.dtype)

    values = tokens_ref[...]
    for i, out in enumerate(outs):
        rows = pick_ref[i * length : (i + 1) * length]
        out[...] = jnp.dot(rows, values, preferred_element_type=jnp.float32).astype(out.dtype)


def dispatch(spread, row_slot, slot, tokens, messages):
    count, width = tokens.shape
    total = spread.shape[0]
    length = total // messages
    step = min(width, 1024)
    return pl.pallas_call(
        dispatch_kernel,
        grid=(width // step,),
        in_specs=[
            pl.BlockSpec(spread.shape, lambda i: (0, 0)),
            pl.BlockSpec(row_slot.shape, lambda i: (0, 0)),
            pl.BlockSpec(slot.shape, lambda i: (0, 0)),
            pl.BlockSpec((count, step), lambda i: (0, i)),
        ],
        out_specs=[pl.BlockSpec((length, step), lambda i: (0, i))] * messages,
        out_shape=[jax.ShapeDtypeStruct((length, width), tokens.dtype)] * messages,
        scratch_shapes=[pltpu.VMEM((total, count), tokens.dtype)],
        cost_estimate=pl.CostEstimate(
            flops=2 * total * count * width,
            bytes_accessed=2 * width * (count + total),
            transcendentals=0,
        ),
        interpret=INTERPRET,
        name="dispatch",
    )(spread, row_slot, slot, tokens)


def expert_kernel(count, place_ref, *refs):
    values, parts, outs = refs[:count], refs[count : count + PARTS], refs[count + PARTS :]
    place, core = place_ref[0], place_ref[1]
    half = parts[0].shape[0]
    for value, out in zip(values, outs):
        total = jnp.zeros(out.shape, jnp.float32)
        for i, part in enumerate(parts):
            side = core if i % 2 == 0 else 1 - core
            start = (lax.rem(place + SHIFTS[i // 2], SIDE) * 2 + side) * half
            span = pl.ds(pl.multiple_of(start, half), half)
            total += jnp.dot(value[:, span], part[...], preferred_element_type=jnp.float32)
        out[...] = total.astype(out.dtype)


def expert(place, values, parts):
    rows, width = values[0].shape
    half, hidden = parts[0].shape
    step = min(hidden, 256)
    left = pl.BlockSpec((rows, width), lambda i: (0, 0))
    right = pl.BlockSpec((half, step), lambda i: (0, i))
    result = pl.BlockSpec((rows, step), lambda i: (0, i))
    return pl.pallas_call(
        functools.partial(expert_kernel, len(values)),
        grid=(hidden // step,),
        in_specs=[pl.BlockSpec(memory_space=pltpu.SMEM)] + [left] * len(values) + [right] * PARTS,
        out_specs=[result] * len(values),
        out_shape=[jax.ShapeDtypeStruct((rows, hidden), values[0].dtype)] * len(values),
        cost_estimate=pl.CostEstimate(
            flops=2 * len(values) * rows * width * hidden,
            bytes_accessed=2 * (len(values) * rows * (width + hidden) + width * hidden),
            transcendentals=0,
        ),
        interpret=INTERPRET,
        name="expert",
    )(place, *values, *parts)


def combine_kernel(count, hi_ref, lo_ref, *refs):
    blocks, base, out_ref, rows_ref = refs[:count], refs[count:-2], refs[-2], refs[-1]
    rows = blocks[0].shape[0]
    for i, block in enumerate(blocks):
        rows_ref[i * rows : (i + 1) * rows] = block[...]
    used = count * rows
    if used < rows_ref.shape[0]:
        rows_ref[used:] = jnp.zeros((rows_ref.shape[0] - used, rows_ref.shape[1]), rows_ref.dtype)
    values = rows_ref[...]
    total = jnp.dot(hi_ref[...], values, preferred_element_type=jnp.float32)
    total += jnp.dot(lo_ref[...], values, preferred_element_type=jnp.float32)
    for other in base:
        total += other[...]
    out_ref[...] = total.astype(out_ref.dtype)


def combine(hi, lo, blocks, base, dtype):
    count, depth = hi.shape
    hidden = blocks[0].shape[1]
    step = min(hidden, 256)
    left = pl.BlockSpec((count, depth), lambda i: (0, 0))
    right = pl.BlockSpec((blocks[0].shape[0], step), lambda i: (0, i))
    sums = pl.BlockSpec((count, step), lambda i: (0, i))
    return pl.pallas_call(
        functools.partial(combine_kernel, len(blocks)),
        grid=(hidden // step,),
        in_specs=[left, left] + [right] * len(blocks) + [sums] * len(base),
        out_specs=sums,
        out_shape=jax.ShapeDtypeStruct((count, hidden), dtype),
        scratch_shapes=[pltpu.VMEM((depth, step), blocks[0].dtype)],
        cost_estimate=pl.CostEstimate(
            flops=4 * count * depth * hidden,
            bytes_accessed=4 * count * (depth + hidden) + 2 * depth * hidden,
            transcendentals=0,
        ),
        interpret=INTERPRET,
        name="combine",
    )(hi, lo, *blocks, *base)


def expert_order(kind):
    y, x = lax.axis_index("y"), lax.axis_index("x")
    ahead = np.repeat([goff for _, goff in BLOCKS], SIDE).astype(np.int32)
    turn = np.tile(np.arange(SIDE), len(BLOCKS)).astype(np.int32)
    first = (jnp.where(kind == 0, x, y) + ahead + SIDE) % SIDE
    second = (jnp.where(kind == 0, y, x) + turn) % SIDE
    group = jnp.where(kind == 0, second * SIDE + first, first * SIDE + second)
    return (CORES * group + kind)[:, None].astype(jnp.float32)


def move(array, moves):
    return lax.ppermute(array, PLANE, moves)


def across(array, moves, axis):
    return lax.ppermute(array, axis, moves)


def compute(tokens, routes, gates, weights):
    rows, _ = tokens.shape
    experts = CORES * SIDE * SIDE
    capacity = 5 * rows // (2 * experts)
    main = capacity - LOOSE
    mine = experts // CORES
    core = lax.axis_index("core")
    place = jnp.stack([lax.axis_index("z"), core])

    kept = lax.dynamic_index_in_dim(weights, core, 0, keepdims=False)
    given = lax.dynamic_index_in_dim(weights, 1 - core, 0, keepdims=False)
    given = across(given, SWAP, "core")
    ways = jnp.concatenate([routes.T.astype(jnp.float32), gates.T])
    other_ways = across(ways, SWAP, "core")
    other_tokens = across(tokens, SWAP, "core")

    parts = []
    for s in range(len(SETS)):
        pair = [kept, given]
        if s:
            pair = [move(part, pairs(1, 0)) for part in pair]
        below = [across(part, UP, "z") for part in pair]
        above = [across(part, back(UP), "z") for part in pair]
        far = [across(below[0], UP, "z"), across(above[1], back(UP), "z")]
        parts.append(pair + below + above + far)

    used = SIDE * capacity
    length = -(-used // 16) * 16
    unit_of = np.full((length,), -1)
    slot_of = np.full((length,), -1)
    unit_of[: SIDE * main] = np.repeat(np.arange(SIDE), main)
    slot_of[: SIDE * main] = np.tile(np.arange(main), SIDE)
    unit_of[SIDE * main : used] = np.repeat(np.arange(SIDE), LOOSE)
    slot_of[SIDE * main : used] = np.tile(np.arange(main, capacity), SIDE)

    def layout(blocks, classes, depth):
        row_expert = np.full((depth,), -1)
        row_slot = np.full((depth,), -2.0, np.float32)
        at = 0
        for kind in range(classes):
            for b in blocks:
                here = slice(at, at + length)
                row_expert[here] = np.where(unit_of >= 0, kind * mine + b * SIDE + unit_of, -1)
                row_slot[here] = np.where(unit_of >= 0, slot_of, -2)
                at += length
        spread = row_expert[:, None] == np.arange(classes * mine)[None, :]
        return jnp.asarray(spread, jnp.bfloat16), jnp.asarray(row_slot)

    earlier = (
        lax.broadcasted_iota(jnp.int32, (rows, rows), 0)
        < lax.broadcasted_iota(jnp.int32, (rows, rows), 1)
    ).astype(jnp.bfloat16)

    def slots(ids, way):
        in_first, in_second = ids == way[0:1], ids == way[1:2]
        named = in_first | in_second
        rank = jnp.dot(named.astype(jnp.bfloat16), earlier, preferred_element_type=jnp.float32)
        slot = jnp.where(named, jnp.minimum(rank, capacity), -1.0).astype(jnp.bfloat16)
        gate = jnp.where(in_first, way[2:3], jnp.where(in_second, way[3:4], 0.0))
        return slot, gate

    ids = expert_order(core)
    slot, gate = slots(jnp.concatenate([ids, expert_order(1 - core)]), ways)
    other_slot, _ = slots(ids, other_ways)

    arrived = {}
    for group in ((1, 3), (0, 2)):
        spread, row_slot = layout(group, 1, len(group) * length)
        for q, (table, values) in enumerate(((slot[:mine], tokens), (other_slot, other_tokens))):
            blocks = dispatch(spread, row_slot[:, None], table, values, len(group))
            for b, block in zip(group, blocks):
                shift = BLOCKS[b][0]
                if shift:
                    block = move(block, pairs(shift, 0))
                arrived[q, b] = block

    shares = []
    high = lax.reduce_precision(gate, 8, 7)
    turned = (((0,), (1,)), ((), ()))
    per_set = len(BLOCKS) // len(SETS)
    for s in range(len(SETS)):
        held = CORES * per_set * length
        spread, row_slot = layout(range(s * per_set, (s + 1) * per_set), CORES, -(-held // 128) * 128)
        at_row = lax.dot_general(slot, spread, turned, preferred_element_type=jnp.float32)
        share = []
        for part in (high, gate - high):
            part = lax.dot_general(
                part.astype(jnp.bfloat16), spread, turned, preferred_element_type=jnp.float32
            )
            share.append(jnp.where(at_row == row_slot[None, :], part, 0.0).astype(jnp.bfloat16))
        shares.append(share)

    total = ()
    for s in range(len(SETS)):
        members = [(q, s * per_set + i) for i in range(per_set) for q in range(CORES)]
        turns = list(regroup([arrived[m] for m in members], main))
        for turn in (1, 3, 2):
            turns[turn] = move(turns[turn], pairs(0, turn))
        if s == 0:
            place, shares = lax.optimization_barrier((place, shares))
        outs = {}
        for group in EXPERT_CALLS[s]:
            outs.update(zip(group, expert(place, [turns[t] for t in group], parts[s])))
        for turn in (1, 3, 2):
            outs[turn] = move(outs[turn], back(pairs(0, turn)))
        blocks = {}
        for (q, b), block in zip(members, regroup([outs[t] for t in range(SIDE)], main)):
            moves = back(pairs(BLOCKS[b][0], 0))
            if q:
                moves = crossed(moves)
            if q or BLOCKS[b][0]:
                block = move(block, moves)
            blocks[q, b] = block
        ordered = [blocks[q, s * per_set + i] for q in range(CORES) for i in range(per_set)]
        last = s == len(SETS) - 1
        total = (combine(*shares[s], ordered, total, jnp.bfloat16 if last else jnp.float32),)
    return total[0]


def solution(mesh):
    seq, _ = mesh.devices.shape
    fine = Mesh(mesh.devices.reshape(seq // CORES, CORES, SIDE, SIDE), ("z",) + PLANE)
    every = ("z",) + PLANE
    return jax.shard_map(
        compute,
        mesh=fine,
        in_specs=(P(every, None), P(every, None), P(every, None), P(("y", "x"), ("z", "core"), None)),
        out_specs=P(every, None),
        check_vma=False,
    )
```

```python
import functools

import jax
import jax.numpy as jnp
import numpy as np
from jax import lax
from jax.experimental import pallas as pl
from jax.experimental.pallas import tpu as pltpu
from jax.sharding import Mesh, PartitionSpec as P

CORES = 2
SIDE = 4
LOOSE = 2
PLANE = ("core", "y", "x")
SETS = (((0, 0), (1, 1)), ((0, -1), (-1, 2)))
BLOCKS = SETS[0] + SETS[1]
EXPERT_CALLS = (((1, 3, 2, 0),), ((1, 3, 2, 0),))
INTERPRET = False


def flat(core, y, x):
    return (core * SIDE + y % SIDE) * SIDE + x % SIDE


def pairs(first, second):
    out = []
    for core in range(CORES):
        dy, dx = (second, first) if core == 0 else (first, second)
        for y in range(SIDE):
            for x in range(SIDE):
                out.append((flat(core, y, x), flat(core, y + dy, x + dx)))
    return out


def crossed(moves):
    side = SIDE * SIDE
    return [(source, (1 - target // side) * side + target % side) for source, target in moves]


def back(moves):
    return [(target, source) for source, target in moves]


SWAP = [(0, 1), (1, 0)]
SHIFTS = (0, SIDE - 1, 1, 2)
PARTS = 2 * SIDE
UP = [(i, (i + 1) % SIDE) for i in range(SIDE)]


def regroup_kernel(main, *refs):
    ins, outs = refs[:SIDE], refs[SIDE:]
    for i, source in enumerate(ins):
        for j, target in enumerate(outs):
            target[i * main : (i + 1) * main] = source[j * main : (j + 1) * main]
    rest = SIDE * main
    for j, target in enumerate(outs):
        tail = [source[rest + j * LOOSE : rest + (j + 1) * LOOSE] for source in ins]
        target[rest:] = jnp.concatenate(tail, axis=0)


def regroup(arrays, main):
    rows, width = arrays[0].shape
    step = min(width, 1024)
    spec = pl.BlockSpec((rows, step), lambda i: (0, i))
    size = SIDE * rows * width * 2
    return pl.pallas_call(
        functools.partial(regroup_kernel, main),
        grid=(width // step,),
        in_specs=[spec] * SIDE,
        out_specs=[spec] * SIDE,
        out_shape=[jax.ShapeDtypeStruct((rows, width), arrays[0].dtype)] * SIDE,
        cost_estimate=pl.CostEstimate(flops=size, bytes_accessed=2 * size, transcendentals=0),
        interpret=INTERPRET,
        name="regroup",
    )(*arrays)


def dispatch_kernel(spread_ref, row_slot_ref, slot_ref, tokens_ref, *refs):
    outs, pick_ref = refs[:-1], refs[-1]
    length = outs[0].shape[0]
    stride = pick_ref.shape[0] // len(outs)

    @pl.when(pl.program_id(0) == 0)
    def _():
        at_row = jnp.dot(spread_ref[...], slot_ref[...], preferred_element_type=jnp.float32)
        pick_ref[...] = jnp.where(at_row == row_slot_ref[...], 1.0, 0.0).astype(pick_ref.dtype)

    values = tokens_ref[...]
    for i, out in enumerate(outs):
        rows = pick_ref[i * stride : (i + 1) * stride]
        block = jnp.dot(rows, values, preferred_element_type=jnp.float32)
        out[...] = block[:length].astype(out.dtype)


def dispatch(spread, row_slot, slot, tokens, messages, length):
    count, width = tokens.shape
    total = spread.shape[0]
    step = min(width, 1024)
    return pl.pallas_call(
        dispatch_kernel,
        grid=(width // step,),
        in_specs=[
            pl.BlockSpec(spread.shape, lambda i: (0, 0)),
            pl.BlockSpec(row_slot.shape, lambda i: (0, 0)),
            pl.BlockSpec(slot.shape, lambda i: (0, 0)),
            pl.BlockSpec((count, step), lambda i: (0, i)),
        ],
        out_specs=[pl.BlockSpec((length, step), lambda i: (0, i))] * messages,
        out_shape=[jax.ShapeDtypeStruct((length, width), tokens.dtype)] * messages,
        scratch_shapes=[pltpu.VMEM((total, count), tokens.dtype)],
        cost_estimate=pl.CostEstimate(
            flops=2 * total * count * width,
            bytes_accessed=2 * width * (count + total),
            transcendentals=0,
        ),
        interpret=INTERPRET,
        name="dispatch",
    )(spread, row_slot, slot, tokens)


def expert_kernel(count, place_ref, *refs):
    values, parts = refs[:count], refs[count : count + PARTS]
    outs, whole_ref = refs[count + PARTS : -1], refs[-1]
    place, core = place_ref[0], place_ref[1]
    half = parts[0].shape[0]
    for i, part in enumerate(parts):
        side = core if i % 2 == 0 else 1 - core
        start = (lax.rem(place + SHIFTS[i // 2], SIDE) * 2 + side) * half
        whole_ref[pl.ds(pl.multiple_of(start, half), half)] = part[...]
    for value, out in zip(values, outs):
        out[...] = jnp.dot(
            value[...], whole_ref[...], preferred_element_type=jnp.float32
        ).astype(out.dtype)


def expert(place, values, parts):
    rows, width = values[0].shape
    half, hidden = parts[0].shape
    step = min(hidden, 256)
    left = pl.BlockSpec((rows, width), lambda i: (0, 0))
    right = pl.BlockSpec((half, step), lambda i: (0, i))
    result = pl.BlockSpec((rows, step), lambda i: (0, i))
    return pl.pallas_call(
        functools.partial(expert_kernel, len(values)),
        grid=(hidden // step,),
        in_specs=[pl.BlockSpec(memory_space=pltpu.SMEM)] + [left] * len(values) + [right] * PARTS,
        out_specs=[result] * len(values),
        out_shape=[jax.ShapeDtypeStruct((rows, hidden), values[0].dtype)] * len(values),
        scratch_shapes=[pltpu.VMEM((width, step), values[0].dtype)],
        cost_estimate=pl.CostEstimate(
            flops=2 * len(values) * rows * width * hidden,
            bytes_accessed=2 * (len(values) * rows * (width + hidden) + width * hidden),
            transcendentals=0,
        ),
        interpret=INTERPRET,
        name="expert",
    )(place, *values, *parts)


def combine_kernel(count, share_ref, *refs):
    blocks, base, out_ref, rows_ref = refs[:count], refs[count:-2], refs[-2], refs[-1]
    rows = blocks[0].shape[0]
    stride = -(-rows // 16) * 16
    rows_ref[...] = jnp.zeros_like(rows_ref)
    for i, block in enumerate(blocks):
        rows_ref[i * stride : i * stride + rows] = block[...]
    both = jnp.dot(share_ref[...], rows_ref[...], preferred_element_type=jnp.float32)
    tokens = out_ref.shape[0]
    total = both[:tokens] + both[tokens:]
    for other in base:
        total += other[...]
    out_ref[...] = total.astype(out_ref.dtype)


def combine(share, blocks, base, dtype):
    depth = share.shape[1]
    count = share.shape[0] // 2
    hidden = blocks[0].shape[1]
    step = min(hidden, 256)
    right = pl.BlockSpec((blocks[0].shape[0], step), lambda i: (0, i))
    sums = pl.BlockSpec((count, step), lambda i: (0, i))
    return pl.pallas_call(
        functools.partial(combine_kernel, len(blocks)),
        grid=(hidden // step,),
        in_specs=[pl.BlockSpec(share.shape, lambda i: (0, 0))] + [right] * len(blocks) + [sums] * len(base),
        out_specs=sums,
        out_shape=jax.ShapeDtypeStruct((count, hidden), dtype),
        scratch_shapes=[pltpu.VMEM((depth, step), blocks[0].dtype)],
        cost_estimate=pl.CostEstimate(
            flops=4 * count * depth * hidden,
            bytes_accessed=4 * count * (depth + hidden) + 2 * depth * hidden,
            transcendentals=0,
        ),
        interpret=INTERPRET,
        name="combine",
    )(share, *blocks, *base)


def expert_order(kind):
    y, x = lax.axis_index("y"), lax.axis_index("x")
    ahead = np.repeat([goff for _, goff in BLOCKS], SIDE).astype(np.int32)
    turn = np.tile(np.arange(SIDE), len(BLOCKS)).astype(np.int32)
    first = (jnp.where(kind == 0, x, y) + ahead + SIDE) % SIDE
    second = (jnp.where(kind == 0, y, x) + turn) % SIDE
    group = jnp.where(kind == 0, second * SIDE + first, first * SIDE + second)
    return (CORES * group + kind)[:, None].astype(jnp.float32)


def move(array, moves):
    return lax.ppermute(array, PLANE, moves)


def across(array, moves, axis):
    return lax.ppermute(array, axis, moves)


def compute(tokens, routes, gates, weights):
    rows, _ = tokens.shape
    experts = CORES * SIDE * SIDE
    capacity = 5 * rows // (2 * experts)
    main = capacity - LOOSE
    mine = experts // CORES
    core = lax.axis_index("core")
    place = jnp.stack([lax.axis_index("z"), core])

    kept = lax.dynamic_index_in_dim(weights, core, 0, keepdims=False)
    given = lax.dynamic_index_in_dim(weights, 1 - core, 0, keepdims=False)
    given = across(given, SWAP, "core")
    ways = jnp.concatenate([routes.T.astype(jnp.float32), gates.T])
    other_ways = across(ways, SWAP, "core")
    other_tokens = across(tokens, SWAP, "core")

    parts = []
    for s in range(len(SETS)):
        pair = [kept, given]
        if s:
            pair = [move(part, pairs(1, 0)) for part in pair]
        below = [across(part, UP, "z") for part in pair]
        above = [across(part, back(UP), "z") for part in pair]
        far = [across(below[0], UP, "z"), across(above[1], back(UP), "z")]
        parts.append(pair + below + above + far)

    used = SIDE * capacity
    length = -(-used // 16) * 16
    unit_of = np.full((length,), -1)
    slot_of = np.full((length,), -1)
    unit_of[: SIDE * main] = np.repeat(np.arange(SIDE), main)
    slot_of[: SIDE * main] = np.tile(np.arange(main), SIDE)
    unit_of[SIDE * main : used] = np.repeat(np.arange(SIDE), LOOSE)
    slot_of[SIDE * main : used] = np.tile(np.arange(main, capacity), SIDE)

    def layout(blocks, classes, depth):
        row_expert = np.full((depth,), -1)
        row_slot = np.full((depth,), -2.0, np.float32)
        at = 0
        for kind in range(classes):
            for b in blocks:
                here = slice(at, at + length)
                row_expert[here] = np.where(unit_of >= 0, kind * mine + b * SIDE + unit_of, -1)
                row_slot[here] = np.where(unit_of >= 0, slot_of, -2)
                at += length
        spread = row_expert[:, None] == np.arange(classes * mine)[None, :]
        return jnp.asarray(spread, jnp.bfloat16), jnp.asarray(row_slot)

    earlier = (
        lax.broadcasted_iota(jnp.int32, (rows, rows), 0)
        < lax.broadcasted_iota(jnp.int32, (rows, rows), 1)
    ).astype(jnp.bfloat16)

    def slots(ids, way):
        in_first, in_second = ids == way[0:1], ids == way[1:2]
        named = in_first | in_second
        rank = jnp.dot(named.astype(jnp.bfloat16), earlier, preferred_element_type=jnp.float32)
        slot = jnp.where(named, jnp.minimum(rank, capacity), -1.0).astype(jnp.bfloat16)
        gate = jnp.where(in_first, way[2:3], jnp.where(in_second, way[3:4], 0.0))
        return slot, gate

    ids = expert_order(core)
    slot, gate = slots(jnp.concatenate([ids, expert_order(1 - core)]), ways)
    other_slot, _ = slots(ids, other_ways)

    arrived = {}
    for group in ((1, 3), (0, 2)):
        spread, row_slot = layout(group, 1, len(group) * length)
        for q, (table, values) in enumerate(((slot[:mine], tokens), (other_slot, other_tokens))):
            blocks = dispatch(spread, row_slot[:, None], table, values, len(group), used)
            for b, block in zip(group, blocks):
                shift = BLOCKS[b][0]
                if shift:
                    block = move(block, pairs(shift, 0))
                arrived[q, b] = block

    shares = []
    high = lax.reduce_precision(gate, 8, 7)
    turned = (((0,), (1,)), ((), ()))
    per_set = len(BLOCKS) // len(SETS)
    for s in range(len(SETS)):
        held = CORES * per_set * length
        spread, row_slot = layout(range(s * per_set, (s + 1) * per_set), CORES, -(-held // 128) * 128)
        at_row = lax.dot_general(slot, spread, turned, preferred_element_type=jnp.float32)
        share = []
        for part in (high, gate - high):
            part = lax.dot_general(
                part.astype(jnp.bfloat16), spread, turned, preferred_element_type=jnp.float32
            )
            share.append(jnp.where(at_row == row_slot[None, :], part, 0.0).astype(jnp.bfloat16))
        shares.append(jnp.concatenate(share))

    total = ()
    for s in range(len(SETS)):
        members = [(q, s * per_set + i) for i in range(per_set) for q in range(CORES)]
        turns = list(regroup([arrived[m] for m in members], main))
        for turn in (1, 3, 2):
            turns[turn] = move(turns[turn], pairs(0, turn))
        if s == 0:
            place, shares = lax.optimization_barrier((place, shares))
        outs = {}
        for group in EXPERT_CALLS[s]:
            outs.update(zip(group, expert(place, [turns[t] for t in group], parts[s])))
        for turn in (1, 3, 2):
            outs[turn] = move(outs[turn], back(pairs(0, turn)))
        grouped = regroup([outs[t] for t in range(SIDE)], main)
        if s == 0:
            first_members, early = members, grouped
        else:
            finish = ((0, first_members, early), (1, members, grouped))
    for s, members, grouped in finish:
        blocks = {}
        for (q, b), block in zip(members, grouped):
            moves = back(pairs(BLOCKS[b][0], 0))
            if q:
                moves = crossed(moves)
            if q or BLOCKS[b][0]:
                block = move(block, moves)
            blocks[q, b] = block
        ordered = [blocks[q, s * per_set + i] for q in range(CORES) for i in range(per_set)]
        last = s == len(SETS) - 1
        total = (combine(shares[s], ordered, total, jnp.bfloat16 if last else jnp.float32),)
    return total[0]


def solution(mesh):
    seq, _ = mesh.devices.shape
    fine = Mesh(mesh.devices.reshape(seq // CORES, CORES, SIDE, SIDE), ("z",) + PLANE)
    every = ("z",) + PLANE
    return jax.shard_map(
        compute,
        mesh=fine,
        in_specs=(P(every, None), P(every, None), P(every, None), P(("y", "x"), ("z", "core"), None)),
        out_specs=P(every, None),
        check_vma=False,
    )
```

```python
import functools

import jax
import jax.numpy as jnp
import numpy as np
from jax import lax
from jax.experimental import pallas as pl
from jax.experimental.pallas import tpu as pltpu
from jax.sharding import Mesh, PartitionSpec as P

CORES = 2
SIDE = 4
LOOSE = 2
PLANE = ("core", "y", "x")
SETS = (((0, 0), (1, 1)), ((0, -1), (-1, 2)))
BLOCKS = SETS[0] + SETS[1]
EXPERT_CALLS = (((1, 3, 2, 0),), ((1, 3, 2, 0),))
SUMS = ((0, 1, 2), (3,))
INTERPRET = False


def flat(core, y, x):
    return (core * SIDE + y % SIDE) * SIDE + x % SIDE


def pairs(first, second):
    out = []
    for core in range(CORES):
        dy, dx = (second, first) if core == 0 else (first, second)
        for y in range(SIDE):
            for x in range(SIDE):
                out.append((flat(core, y, x), flat(core, y + dy, x + dx)))
    return out


def crossed(moves):
    side = SIDE * SIDE
    return [(source, (1 - target // side) * side + target % side) for source, target in moves]


def back(moves):
    return [(target, source) for source, target in moves]


SWAP = [(0, 1), (1, 0)]
SHIFTS = (0, SIDE - 1, 1, 2)
PARTS = 2 * SIDE
UP = [(i, (i + 1) % SIDE) for i in range(SIDE)]


def regroup_kernel(main, *refs):
    ins, outs = refs[:SIDE], refs[SIDE:]
    for i, source in enumerate(ins):
        for j, target in enumerate(outs):
            target[i * main : (i + 1) * main] = source[j * main : (j + 1) * main]
    rest = SIDE * main
    for j, target in enumerate(outs):
        tail = [source[rest + j * LOOSE : rest + (j + 1) * LOOSE] for source in ins]
        target[rest:] = jnp.concatenate(tail, axis=0)


def regroup(arrays, main):
    rows, width = arrays[0].shape
    step = min(width, 1024)
    spec = pl.BlockSpec((rows, step), lambda i: (0, i))
    size = SIDE * rows * width * 2
    return pl.pallas_call(
        functools.partial(regroup_kernel, main),
        grid=(width // step,),
        in_specs=[spec] * SIDE,
        out_specs=[spec] * SIDE,
        out_shape=[jax.ShapeDtypeStruct((rows, width), arrays[0].dtype)] * SIDE,
        cost_estimate=pl.CostEstimate(flops=size, bytes_accessed=2 * size, transcendentals=0),
        interpret=INTERPRET,
        compiler_params=pltpu.CompilerParams(vmem_limit_bytes=6 * SIDE * step * rows * 2 + (4 << 20)),
        name="regroup",
    )(*arrays)


def dispatch_kernel(spread_ref, row_slot_ref, slot_ref, tokens_ref, *refs):
    outs, pick_ref = refs[:-1], refs[-1]
    length = outs[0].shape[0]
    stride = pick_ref.shape[0] // len(outs)

    @pl.when(pl.program_id(0) == 0)
    def _():
        at_row = jnp.dot(spread_ref[...], slot_ref[...], preferred_element_type=jnp.float32)
        pick_ref[...] = jnp.where(at_row == row_slot_ref[...], 1.0, 0.0).astype(pick_ref.dtype)

    values = tokens_ref[...]
    for i, out in enumerate(outs):
        rows = pick_ref[i * stride : (i + 1) * stride]
        block = jnp.dot(rows, values, preferred_element_type=jnp.float32)
        out[...] = block[:length].astype(out.dtype)


def dispatch(spread, row_slot, slot, tokens, messages, length):
    count, width = tokens.shape
    total = spread.shape[0]
    step = min(width, 1024)
    return pl.pallas_call(
        dispatch_kernel,
        grid=(width // step,),
        in_specs=[
            pl.BlockSpec(spread.shape, lambda i: (0, 0)),
            pl.BlockSpec(row_slot.shape, lambda i: (0, 0)),
            pl.BlockSpec(slot.shape, lambda i: (0, 0)),
            pl.BlockSpec((count, step), lambda i: (0, i)),
        ],
        out_specs=[pl.BlockSpec((length, step), lambda i: (0, i))] * messages,
        out_shape=[jax.ShapeDtypeStruct((length, width), tokens.dtype)] * messages,
        scratch_shapes=[pltpu.VMEM((total, count), tokens.dtype)],
        cost_estimate=pl.CostEstimate(
            flops=2 * total * count * width,
            bytes_accessed=2 * width * (count + total),
            transcendentals=0,
        ),
        interpret=INTERPRET,
        compiler_params=pltpu.CompilerParams(vmem_limit_bytes=12 << 20),
        name="dispatch",
    )(spread, row_slot, slot, tokens)


def expert_kernel(count, place_ref, *refs):
    values, parts = refs[:count], refs[count : count + PARTS]
    outs, whole_ref = refs[count + PARTS : -1], refs[-1]
    place, core = place_ref[0], place_ref[1]
    half = parts[0].shape[0]
    for i, part in enumerate(parts):
        side = core if i % 2 == 0 else 1 - core
        start = (lax.rem(place + SHIFTS[i // 2], SIDE) * 2 + side) * half
        whole_ref[pl.ds(pl.multiple_of(start, half), half)] = part[...]
    for value, out in zip(values, outs):
        out[...] = jnp.dot(
            value[...], whole_ref[...], preferred_element_type=jnp.float32
        ).astype(out.dtype)


def expert(place, values, parts):
    rows, width = values[0].shape
    half, hidden = parts[0].shape
    step = min(hidden, 256)
    left = pl.BlockSpec((rows, width), lambda i: (0, 0))
    right = pl.BlockSpec((half, step), lambda i: (0, i))
    result = pl.BlockSpec((rows, step), lambda i: (0, i))
    return pl.pallas_call(
        functools.partial(expert_kernel, len(values)),
        grid=(hidden // step,),
        in_specs=[pl.BlockSpec(memory_space=pltpu.SMEM)] + [left] * len(values) + [right] * PARTS,
        out_specs=[result] * len(values),
        out_shape=[jax.ShapeDtypeStruct((rows, hidden), values[0].dtype)] * len(values),
        scratch_shapes=[pltpu.VMEM((width, step), values[0].dtype)],
        cost_estimate=pl.CostEstimate(
            flops=2 * len(values) * rows * width * hidden,
            bytes_accessed=2 * (len(values) * rows * (width + hidden) + width * hidden),
            transcendentals=0,
        ),
        interpret=INTERPRET,
        compiler_params=pltpu.CompilerParams(vmem_limit_bytes=26 << 20),
        name="expert",
    )(place, *values, *parts)


def combine_kernel(count, share_ref, *refs):
    blocks, base, out_ref, rows_ref = refs[:count], refs[count:-2], refs[-2], refs[-1]
    rows = blocks[0].shape[0]
    stride = -(-rows // 16) * 16

    @pl.when(pl.program_id(0) == 0)
    def _():
        rows_ref[...] = jnp.zeros_like(rows_ref)
        for i, block in enumerate(blocks):
            rows_ref[i * stride : i * stride + rows] = block[...]

    total = jnp.dot(share_ref[0], rows_ref[...], preferred_element_type=jnp.float32)
    total += jnp.dot(share_ref[1], rows_ref[...], preferred_element_type=jnp.float32)
    for other in base:
        total += other[...]
    out_ref[...] = total.astype(out_ref.dtype)


def combine(share, blocks, base, dtype):
    _, count, depth = share.shape
    hidden = blocks[0].shape[1]
    step = count // 4
    right = pl.BlockSpec(blocks[0].shape, lambda i: (0, 0))
    sums = pl.BlockSpec((step, hidden), lambda i: (i, 0))
    left = pl.BlockSpec((2, step, depth), lambda i: (0, i, 0))
    return pl.pallas_call(
        functools.partial(combine_kernel, len(blocks)),
        grid=(count // step,),
        in_specs=[left] + [right] * len(blocks) + [sums] * len(base),
        out_specs=sums,
        out_shape=jax.ShapeDtypeStruct((count, hidden), dtype),
        scratch_shapes=[pltpu.VMEM((depth, hidden), blocks[0].dtype)],
        cost_estimate=pl.CostEstimate(
            flops=4 * count * depth * hidden,
            bytes_accessed=4 * count * (depth + hidden) + 2 * depth * hidden,
            transcendentals=0,
        ),
        interpret=INTERPRET,
        compiler_params=pltpu.CompilerParams(vmem_limit_bytes=32 << 20),
        name="combine",
    )(share, *blocks, *base)


def expert_order(kind):
    y, x = lax.axis_index("y"), lax.axis_index("x")
    ahead = np.repeat([goff for _, goff in BLOCKS], SIDE).astype(np.int32)
    turn = np.tile(np.arange(SIDE), len(BLOCKS)).astype(np.int32)
    first = (jnp.where(kind == 0, x, y) + ahead + SIDE) % SIDE
    second = (jnp.where(kind == 0, y, x) + turn) % SIDE
    group = jnp.where(kind == 0, second * SIDE + first, first * SIDE + second)
    return (CORES * group + kind)[:, None].astype(jnp.float32)


def move(array, moves):
    return lax.ppermute(array, PLANE, moves)


def across(array, moves, axis):
    return lax.ppermute(array, axis, moves)


def compute(tokens, routes, gates, weights):
    rows, _ = tokens.shape
    experts = CORES * SIDE * SIDE
    capacity = 5 * rows // (2 * experts)
    main = capacity - LOOSE
    mine = experts // CORES
    core = lax.axis_index("core")
    place = jnp.stack([lax.axis_index("z"), core])

    kept = lax.dynamic_index_in_dim(weights, core, 0, keepdims=False)
    given = lax.dynamic_index_in_dim(weights, 1 - core, 0, keepdims=False)
    given = across(given, SWAP, "core")
    ways = jnp.concatenate([routes.T.astype(jnp.float32), gates.T])
    other_ways = across(ways, SWAP, "core")
    other_tokens = across(tokens, SWAP, "core")

    parts = []
    for s in range(len(SETS)):
        pair = [kept, given]
        if s:
            pair = [move(part, pairs(1, 0)) for part in pair]
        below = [across(part, UP, "z") for part in pair]
        above = [across(part, back(UP), "z") for part in pair]
        far = [across(below[0], UP, "z"), across(above[1], back(UP), "z")]
        parts.append(pair + below + above + far)

    used = SIDE * capacity
    length = -(-used // 16) * 16
    unit_of = np.full((length,), -1)
    slot_of = np.full((length,), -1)
    unit_of[: SIDE * main] = np.repeat(np.arange(SIDE), main)
    slot_of[: SIDE * main] = np.tile(np.arange(main), SIDE)
    unit_of[SIDE * main : used] = np.repeat(np.arange(SIDE), LOOSE)
    slot_of[SIDE * main : used] = np.tile(np.arange(main, capacity), SIDE)

    def layout(blocks, classes, depth):
        row_expert = np.full((depth,), -1)
        row_slot = np.full((depth,), -2.0, np.float32)
        at = 0
        for kind in range(classes):
            for b in blocks:
                here = slice(at, at + length)
                row_expert[here] = np.where(unit_of >= 0, kind * mine + b * SIDE + unit_of, -1)
                row_slot[here] = np.where(unit_of >= 0, slot_of, -2)
                at += length
        spread = row_expert[:, None] == np.arange(classes * mine)[None, :]
        return jnp.asarray(spread, jnp.bfloat16), jnp.asarray(row_slot)

    earlier = (
        lax.broadcasted_iota(jnp.int32, (rows, rows), 0)
        < lax.broadcasted_iota(jnp.int32, (rows, rows), 1)
    ).astype(jnp.bfloat16)

    def slots(ids, way):
        in_first, in_second = ids == way[0:1], ids == way[1:2]
        named = in_first | in_second
        rank = jnp.dot(named.astype(jnp.bfloat16), earlier, preferred_element_type=jnp.float32)
        slot = jnp.where(named, jnp.minimum(rank, capacity), -1.0).astype(jnp.bfloat16)
        gate = jnp.where(in_first, way[2:3], jnp.where(in_second, way[3:4], 0.0))
        return slot, gate

    ids = expert_order(core)
    slot, gate = slots(jnp.concatenate([ids, expert_order(1 - core)]), ways)
    other_slot, _ = slots(ids, other_ways)

    arrived = {}
    for group in ((1, 3), (0, 2)):
        spread, row_slot = layout(group, 1, len(group) * length)
        for q, (table, values) in enumerate(((slot[:mine], tokens), (other_slot, other_tokens))):
            blocks = dispatch(spread, row_slot[:, None], table, values, len(group), used)
            for b, block in zip(group, blocks):
                shift = BLOCKS[b][0]
                if shift:
                    block = move(block, pairs(shift, 0))
                arrived[q, b] = block

    shares = []
    high = lax.reduce_precision(gate, 8, 7)
    turned = (((0,), (1,)), ((), ()))
    per_set = len(BLOCKS) // len(SETS)
    for group in SUMS:
        held = CORES * len(group) * length
        spread, row_slot = layout(group, CORES, -(-held // 128) * 128)
        at_row = lax.dot_general(slot, spread, turned, preferred_element_type=jnp.float32)
        share = []
        for part in (high, gate - high):
            part = lax.dot_general(
                part.astype(jnp.bfloat16), spread, turned, preferred_element_type=jnp.float32
            )
            share.append(jnp.where(at_row == row_slot[None, :], part, 0.0).astype(jnp.bfloat16))
        shares.append(jnp.stack(share))

    total = ()
    for s in range(len(SETS)):
        members = [(q, s * per_set + i) for i in range(per_set) for q in range(CORES)]
        turns = list(regroup([arrived[m] for m in members], main))
        for turn in (1, 3, 2):
            turns[turn] = move(turns[turn], pairs(0, turn))
        if s == 0:
            place, shares = lax.optimization_barrier((place, shares))
        outs = {}
        for group in EXPERT_CALLS[s]:
            outs.update(zip(group, expert(place, [turns[t] for t in group], parts[s])))
        for turn in (1, 3, 2):
            outs[turn] = move(outs[turn], back(pairs(0, turn)))
        grouped = regroup([outs[t] for t in range(SIDE)], main)
        if s == 0:
            first_members, early = members, grouped
        else:
            finish = ((first_members, early), (members, grouped))
    blocks = {}
    for members, grouped in finish:
        for (q, b), block in zip(members, grouped):
            moves = back(pairs(BLOCKS[b][0], 0))
            if q:
                moves = crossed(moves)
            if q or BLOCKS[b][0]:
                block = move(block, moves)
            blocks[q, b] = block
    for i, group in enumerate(SUMS):
        ordered = [blocks[q, b] for q in range(CORES) for b in group]
        kind = jnp.bfloat16 if i == len(SUMS) - 1 else jnp.float32
        total = (combine(shares[i], ordered, total, kind),)
    return total[0]


def solution(mesh):
    seq, _ = mesh.devices.shape
    fine = Mesh(mesh.devices.reshape(seq // CORES, CORES, SIDE, SIDE), ("z",) + PLANE)
    every = ("z",) + PLANE
    return jax.shard_map(
        compute,
        mesh=fine,
        in_specs=(P(every, None), P(every, None), P(every, None), P(("y", "x"), ("z", "core"), None)),
        out_specs=P(every, None),
        check_vma=False,
    )
```
